32 devices in a mesh: obj: 8 (over y, x, core), img: 4 (over z).
Axes of the slice: x: 2, y: 2, z: 4, core: 2. Of those that a mesh axis runs over, the one named last changes fastest.
Arguments:
- tri_planes: bfloat16 [2, 8, 1024, 1024], P(None, 'obj', 'img'), may hold values from -6 to 6
- images: bfloat16 [2, 8, 1024, 768], P(None, 'obj', 'img'), may hold values from -6 to 6
- cameras: float32 [16, 20], replicated, may hold values from -4 to 4
- cam_index: int32 [16], replicated, may hold values from 0 to 15, each once
- w_mod: bfloat16 [20, 6144], replicated, may hold values from -0.5 to 0.5
- w_query: bfloat16 [1024, 1024], replicated, may hold values from -0.375 to 0.375
- w_kv_image: bfloat16 [768, 2048], replicated, may hold values from -0.21875 to 0.21875
- w_cross_out: bfloat16 [1024, 1024], replicated, may hold values from -0.75 to 0.75
- w_qkv: bfloat16 [1024, 3072], replicated, may hold values from -0.25 to 0.25
- w_self_out: bfloat16 [1024, 1024], replicated, may hold values from -0.75 to 0.75
- w_up: bfloat16 [1024, 4096], replicated, may hold values from -0.1875 to 0.1875
- w_down: bfloat16 [4096, 1024], replicated, may hold values from -0.09375 to 0.09375
- cotangent: bfloat16 [2, 8, 1024, 1024], P(None, 'obj', 'img'), may hold values from -6 to 6
Outputs:
- out: bfloat16 [2, 8, 1024, 1024], P(None, 'obj', 'img')
- grad_tri: float32 [2, 8, 1024, 1024], P(None, 'obj', 'img')
- grad_images: float32 [2, 8, 1024, 768], P(None, 'obj', 'img')
- grad_w_mod: float32 [20, 6144], P(None, 'obj')
- grad_w_query: float32 [1024, 1024], P('obj')
- grad_w_kv_image: float32 [768, 2048], P('obj')
- grad_w_cross_out: float32 [1024, 1024], P('obj')
- grad_w_qkv: float32 [1024, 3072], P('obj')
- grad_w_self_out: float32 [1024, 1024], P('obj')
- grad_w_up: float32 [1024, 4096], P('obj')
- grad_w_down: float32 [4096, 1024], P('obj')
The draws below stay inside these ranges and needn't reach their ends.
Inputs may be any that keep to these rules, and one draw needn't show every extreme that they name: cam_index names each of the 16 camera rows exactly once.
All inputs are finite; a program needn't handle non-finite values.
Results may differ from the reference program's by a relative error of at most 0.029.
The reference program's roundings to bfloat16 on the way count: a program that leaves them out, or rounds other values in their place, can miss the bound.
Values may be sent and summed in bfloat16 or wider, within the bound.
A program may use at most 256 MiB of HBM per device.

```python
import jax
import jax.numpy as jnp
from jax import lax

D = 1024
H = 16
HD = 64
F = 4096
DI = 768
CAM = 20
MICRO = 2
GROUPS = 8
OBJECTS = 16
TRI_LEN = 1024
IMG_LEN = 1024


def block_scale(key, dims, cuts, smallest, high):
    loudness, own = 1.0, jax.random.fold_in(key, 6)
    for dim, parts in cuts:
        draws = jnp.exp(jax.random.uniform(jax.random.fold_in(own, dim), (parts,), jnp.float32, smallest / len(cuts), high / len(cuts)))
        loudness = loudness * jnp.repeat(draws, dims[dim] // parts).reshape([-1 if axis == dim else 1 for axis in range(len(dims))])
    return loudness


def gaussian(stream_key, shape, deviation, bound, cuts=(), dtype=jnp.bfloat16):
    gain = block_scale(stream_key, shape, cuts, -0.22, 0.18) if cuts else 1.0
    array = jax.random.normal(stream_key, shape, jnp.float32) * deviation * gain
    return jnp.minimum(jnp.maximum(array, -bound), bound).astype(dtype)


def setup_inputs(seed: int = 0) -> dict:
    splits = jax.random.split(jax.random.key(seed), 14)
    return {
        "tri_planes": gaussian(splits[0], (MICRO, GROUPS, TRI_LEN, D), 1.0, 6.0, ((1, 8), (2, 4))),
        "images": gaussian(splits[1], (MICRO, GROUPS, IMG_LEN, DI), 1.0, 6.0, ((1, 8), (2, 4))),
        "cameras": gaussian(splits[2], (OBJECTS, CAM), 1.0, 4.0, (), jnp.float32),
        "cam_index": jax.random.permutation(splits[3], OBJECTS).astype(jnp.int32),
        "w_mod": gaussian(splits[4], (CAM, 6 * D), (CAM * 8) ** -0.5, 0.5),
        "w_query": gaussian(splits[5], (D, D), (D // 4) ** -0.5, 0.375),
        "w_kv_image": gaussian(splits[6], (DI, 2 * D), DI ** -0.5, 0.21875),
        "w_cross_out": gaussian(splits[7], (D, D), (D // 16) ** -0.5, 0.75),
        "w_qkv": gaussian(splits[8], (D, 3 * D), (D // 2) ** -0.5, 0.25),
        "w_self_out": gaussian(splits[9], (D, D), (D // 16) ** -0.5, 0.75),
        "w_up": gaussian(splits[10], (D, F), D ** -0.5, 0.1875),
        "w_down": gaussian(splits[11], (F, D), F ** -0.5, 0.09375),
        "cotangent": gaussian(splits[12], (MICRO, GROUPS, TRI_LEN, D), 1.0, 6.0, ((1, 8), (2, 4))),
    }


epsilon = 1e-06

@jax.custom_vjp
def low(v):
    return lax.optimization_barrier(v.astype(jnp.bfloat16)).astype(jnp.float32)

@jax.custom_vjp
def low_back(v):
    return v

def low_keep(v):
    return (low(v), None)

def low_pass(kept, grad):
    return (grad,)

def back_keep(v):
    return (v, None)

def back_low(kept, grad):
    return (low(grad),)
low.defvjp(low_keep, low_pass)
low_back.defvjp(back_keep, back_low)

def precise(former, latter):
    return jnp.dot(former, latter, precision=lax.Precision.HIGHEST, preferred_element_type=jnp.float32)

def round_both(value):
    return low_back(low(value))

def modnorm(stream, shift_vec, scale_vec):
    row_mean = lax.optimization_barrier(jnp.mean(stream, axis=-1, keepdims=True))
    centered = stream - row_mean
    variance = lax.optimization_barrier(jnp.mean(centered * centered, axis=-1, keepdims=True))
    return centered * lax.rsqrt(variance + epsilon) * (1.0 + scale_vec) + shift_vec

def gelu_tanh(value):
    return jax.nn.gelu(value, approximate=True)

def attention(queries, keys_values):
    row_count = queries.shape[0]
    key_count = keys_values.shape[0]
    block_rows = min(512, row_count)
    key_heads = keys_values[:, :D].reshape(key_count, H, HD)
    value_heads = keys_values[:, D:].reshape(key_count, H, HD)

    def query_block(block):
        query_heads = block.reshape(block_rows, H, HD)
        scores = jnp.einsum('qhd,khd->hqk', query_heads, key_heads, precision=lax.Precision.HIGHEST) * HD ** (-0.5)
        scores = low_back(scores)
        probabilities = low(jax.nn.softmax(scores, axis=-1))
        attended = jnp.einsum('hqk,khd->qhd', probabilities, value_heads, precision=lax.Precision.HIGHEST)
        return attended.reshape(block_rows, H * HD)
    blocks = queries.reshape(row_count // block_rows, block_rows, H * HD)
    attended = lax.map(jax.checkpoint(query_block), blocks)
    return round_both(attended.reshape(row_count, H * HD))

def block_forward(stream, image_tokens, camera, w_mod, w_query, w_kv_image, w_cross_out, w_qkv, w_self_out, w_up, w_down):
    modulation = precise(camera[None, :], w_mod)[0]
    pieces = [modulation[position * D:(position + 1) * D] for position in range(6)]
    hidden_one = low(modnorm(stream, pieces[0], pieces[1]))
    query_one = round_both(precise(hidden_one, w_query))
    pairs_one = round_both(precise(image_tokens, w_kv_image))
    mixed_one = attention(query_one, pairs_one)
    stream_one = stream + low_back(precise(mixed_one, w_cross_out))
    hidden_two = low(modnorm(stream_one, pieces[2], pieces[3]))
    joined = round_both(precise(hidden_two, w_qkv))
    mixed_two = attention(joined[:, :D], joined[:, D:])
    stream_two = stream_one + low_back(precise(mixed_two, w_self_out))
    hidden_three = low(modnorm(stream_two, pieces[4], pieces[5]))
    upper = low_back(precise(hidden_three, w_up))
    activated = low(gelu_tanh(upper))
    return stream_two + low_back(precise(activated, w_down))

def reference(tri_planes, images, cameras, cam_index, w_mod, w_query, w_kv_image, w_cross_out, w_qkv, w_self_out, w_up, w_down, cotangent):
    planes_flat = tri_planes.reshape(OBJECTS, TRI_LEN, D)
    images_flat = images.reshape(OBJECTS, IMG_LEN, DI)
    cot_flat = cotangent.reshape(OBJECTS, TRI_LEN, D)
    picked = cameras[cam_index]
    weights = (w_mod.astype(jnp.float32), w_query.astype(jnp.float32), w_kv_image.astype(jnp.float32), w_cross_out.astype(jnp.float32), w_qkv.astype(jnp.float32), w_self_out.astype(jnp.float32), w_up.astype(jnp.float32), w_down.astype(jnp.float32))

    def per_object(accumulated, inputs_one):
        stream, image_tokens, camera, cot_one = inputs_one

        def forward_one(stream_in, image_in, *weight_list):
            return block_forward(stream_in, image_in, camera, *weight_list)
        result, pullback = jax.vjp(forward_one, stream.astype(jnp.float32), image_tokens.astype(jnp.float32), *weights)
        gradients = pullback(cot_one.astype(jnp.float32))
        accumulated = tuple((former + latter for former, latter in zip(accumulated, gradients[2:])))
        return (accumulated, (result.astype(jnp.bfloat16), gradients[0], gradients[1]))
    zeros_init = tuple((jnp.zeros(weight.shape, jnp.float32) for weight in weights))
    totals, (outputs, plane_grads, image_grads) = lax.scan(per_object, zeros_init, (planes_flat, images_flat, picked, cot_flat))
    return (outputs.reshape(MICRO, GROUPS, TRI_LEN, D), plane_grads.reshape(MICRO, GROUPS, TRI_LEN, D), image_grads.reshape(MICRO, GROUPS, IMG_LEN, DI), totals[0], totals[1], totals[2], totals[3], totals[4], totals[5], totals[6], totals[7])
```

```python
import functools

import jax
import jax.numpy as jnp
from jax import lax
from jax.experimental import pallas as pl
from jax.experimental.pallas import tpu as pltpu
from jax.sharding import PartitionSpec as P

H = 16
HD = 64
BF = jnp.bfloat16
F32 = jnp.float32
AXES = ("obj", "img")

epsilon = 1e-06


def dot(a, b, ca, cb):
    return lax.dot_general(a, b, (((ca,), (cb,)), ((), ())), preferred_element_type=F32)


def modnorm(stream, shift_vec, scale_vec):
    row_mean = jnp.mean(stream, axis=-1, keepdims=True)
    centered = stream - row_mean
    variance = jnp.mean(centered * centered, axis=-1, keepdims=True)
    return centered * lax.rsqrt(variance + epsilon) * (1.0 + scale_vec) + shift_vec


def gelu_tanh(value):
    return jax.nn.gelu(value, approximate=True)


def attend_kernel(q_ref, k0_ref, k1_ref, v0_ref, v1_ref, o_ref, l_ref, *, tq):
    lane = lax.broadcasted_iota(jnp.int32, (1, 128), 1)
    first = lane < HD
    k = jnp.concatenate([k0_ref[...], k1_ref[...]], 0)
    v = jnp.concatenate([v0_ref[...], v1_ref[...]], 0)
    vext = jnp.concatenate([v, jnp.ones(v.shape, BF)], 1)
    for c in range(q_ref.shape[0] // tq):
        rows = slice(c * tq, (c + 1) * tq)
        qc = q_ref[rows, :] * BF(HD**-0.5)
        outs = []
        logs = []
        for h in range(2):
            qm = jnp.where(first if h == 0 else ~first, qc, BF(0))
            s = dot(qm, k, 1, 1)
            m = jnp.max(s, -1, keepdims=True)
            e = jnp.exp(s - m).astype(BF)
            both = dot(e, vext, 1, 0)
            total = both[:, 128:]
            outs.append(both[:, :128] / total)
            logs.append(m + jnp.log(total))
        o_ref[rows, :] = jnp.where(first, outs[0], outs[1]).astype(BF)
        l_ref[rows, :] = jnp.where(first, logs[0], logs[1])


def attend(q, own, other, tq=128):
    t, d = q.shape
    keys = own.shape[0] + other.shape[0]
    pairs = d // 128
    half = lambda off: pl.BlockSpec((own.shape[0], 128), lambda j: (0, j + off))
    col = pl.BlockSpec((t, 128), lambda j: (0, j))
    return pl.pallas_call(
        functools.partial(attend_kernel, tq=min(tq, t)),
        grid=(pairs,),
        in_specs=[col, half(0), half(0), half(pairs), half(pairs)],
        out_specs=[col, col],
        out_shape=[jax.ShapeDtypeStruct((t, d), BF), jax.ShapeDtypeStruct((t, d), F32)],
        compiler_params=pltpu.CompilerParams(vmem_limit_bytes=56 << 20),
        cost_estimate=pl.CostEstimate(
            flops=16 * t * keys * d, bytes_accessed=8 * t * d + 4 * keys * d, transcendentals=t * keys * H
        ),
        name="attend",
    )(q, own, other, own, other)


def attend_back_kernel(
    q_ref, k0_ref, k1_ref, v0_ref, v1_ref, o_ref, g_ref, l_ref,
    dq_ref, dk0_ref, dk1_ref, dv0_ref, dv1_ref, dk_acc, dv_acc, *, tq
):
    lane = lax.broadcasted_iota(jnp.int32, (1, 128), 1)
    first = lane < HD
    k = jnp.concatenate([k0_ref[...], k1_ref[...]], 0)
    v = jnp.concatenate([v0_ref[...], v1_ref[...]], 0)
    kt = k.T
    n0 = k0_ref.shape[0]
    steps = q_ref.shape[0] // tq
    for c in range(steps):
        rows = slice(c * tq, (c + 1) * tq)
        qc = q_ref[rows, :] * BF(HD**-0.5)
        gc = g_ref[rows, :]
        lc = l_ref[rows, :]
        prod = o_ref[rows, :].astype(F32) * gc.astype(F32)
        qt = qc.T
        gt = gc.T
        dqs, dks, dvs = [], [], []
        for h in range(2):
            keep = first if h == 0 else ~first
            head = slice(HD * h, HD * h + HD)
            qm = jnp.where(keep, qc, BF(0))
            gm = jnp.where(keep, gc, BF(0))
            delta = jnp.sum(jnp.where(keep, prod, 0.0), -1, keepdims=True)
            s = dot(qm, k, 1, 1)
            p = jnp.exp(s - lc[:, HD * h : HD * h + 1])
            dp = dot(gm, v, 1, 1)
            ds = (p * (dp - delta)).astype(BF)
            dqs.append(dot(kt[head], ds, 1, 1))
            dks.append(dot(qt[head], ds, 1, 0))
            dvs.append(dot(gt[head], p.astype(BF), 1, 0))
        dq_ref[rows, :] = (jnp.concatenate(dqs, 0) * HD**-0.5).T.astype(BF)
        dk = jnp.concatenate(dks, 0)
        dv = jnp.concatenate(dvs, 0)
        if c == 0:
            dk_acc[...] = dk
            dv_acc[...] = dv
        else:
            dk_acc[...] += dk
            dv_acc[...] += dv
    dk = dk_acc[...].T.astype(BF)
    dv = dv_acc[...].T.astype(BF)
    dk0_ref[...] = dk[:n0]
    dk1_ref[...] = dk[n0:]
    dv0_ref[...] = dv[:n0]
    dv1_ref[...] = dv[n0:]


def attend_back(q, own, other, o, g, logs, tq=256):
    t, d = q.shape
    n0 = own.shape[0]
    keys = 2 * n0
    pairs = d // 128
    half = lambda off: pl.BlockSpec((n0, 128), lambda j: (0, j + off))
    col = pl.BlockSpec((t, 128), lambda j: (0, j))
    return pl.pallas_call(
        functools.partial(attend_back_kernel, tq=min(tq, t)),
        grid=(pairs,),
        in_specs=[col, half(0), half(0), half(pairs), half(pairs), col, col, col],
        out_specs=[col, half(0), half(0), half(0), half(0)],
        out_shape=[jax.ShapeDtypeStruct((t, d), BF)] + [jax.ShapeDtypeStruct((n0, d), BF)] * 4,
        scratch_shapes=[pltpu.VMEM((128, keys), F32)] * 2,
        compiler_params=pltpu.CompilerParams(vmem_limit_bytes=56 << 20),
        cost_estimate=pl.CostEstimate(
            flops=32 * t * keys * d, bytes_accessed=12 * t * d + 8 * keys * d, transcendentals=t * keys * H
        ),
        name="attend_back",
    )(q, own, other, own, other, o, g, logs)


def flat_permute(value, pairs):
    return lax.ppermute(value, AXES, pairs)


def swap_bit(value, bit, groups):
    return lax.ppermute(value, "obj", [(i, i ^ (1 << bit)) for i in range(groups)])


def home_pairs(step, groups, depth):
    pairs = []
    for n in range(groups):
        for z in range(depth):
            core = n % 2
            micro = (z + step) % 2
            pairs.append((n * depth + z, (n - core + z // 2) * depth + micro * 2 + core))
    return pairs


def sum_rows(former, latter, order, groups, group_index):
    tokens, rows = former.shape
    columns = latter.shape[1]
    bits = groups.bit_length() - 1
    own = rows // groups
    shaped = former.reshape((tokens, groups // 2, 2, own))
    side = group_index % 2
    there = lax.dynamic_index_in_dim(shaped, 1 - side, 2, False).reshape(tokens, rows // 2)
    here = lax.dynamic_index_in_dim(shaped, side, 2, False).reshape(tokens, rows // 2)
    arrived = swap_bit(dot(there, latter, 0, 0).astype(BF), 0, groups)
    part = (dot(here, latter, 0, 0) + arrived.astype(F32)).astype(BF)
    left = list(range(bits - 1, 0, -1))
    rest = list(range(1, bits))
    if order:
        rest = rest[::-1]
    for bit in rest:
        place = left.index(bit)
        size = part.shape[0] * part.shape[1] if part.ndim > 2 else part.shape[0]
        part = part.reshape(2**place, 2, size // 2 ** (place + 1), columns)
        side = (group_index >> bit) % 2
        sent = lax.dynamic_index_in_dim(part, 1 - side, 1, False)
        kept = lax.dynamic_index_in_dim(part, side, 1, False)
        arrived = swap_bit(sent, bit, groups)
        part = (kept.astype(F32) + arrived.astype(F32)).astype(BF)
        left.remove(bit)
    return part.reshape(own, columns)


def swap_level(value, bit, depth):
    return lax.ppermute(value, "img", [(i, i ^ (1 << bit)) for i in range(depth)])


def sum_levels(part, level, depth):
    rows, columns = part.shape
    bits = depth.bit_length() - 1
    for bit in range(bits):
        lower, upper = jnp.split(part, 2, 0)
        side = (level >> bit) % 2 == 0
        sent = jnp.where(side, upper, lower)
        kept = jnp.where(side, lower, upper)
        part = (kept.astype(F32) + swap_level(sent, bit, depth).astype(F32)).astype(BF)
    for bit in range(bits)[::-1]:
        side = (level >> bit) % 2 == 0
        arrived = swap_level(part, bit, depth)
        part = jnp.concatenate([jnp.where(side, part, arrived), jnp.where(side, arrived, part)], 0)
    return part.astype(F32)


def local(
    tri_planes,
    images,
    cameras,
    cam_index,
    w_mod,
    w_query,
    w_kv_image,
    w_cross_out,
    w_qkv,
    w_self_out,
    w_up,
    w_down,
    cotangent,
):
    width = w_query.shape[0]
    object_count = cameras.shape[0]
    groups = lax.axis_size("obj")
    depth = lax.axis_size("img")
    n = lax.axis_index("obj")
    z = lax.axis_index("img")
    micros = tri_planes.shape[0]
    assert micros == 2 and depth == 4
    there = [home_pairs(step, groups, depth) for step in range(2)]
    back = [[(b, a) for a, b in pairs] for pairs in there]

    def bring(array):
        blocks = [
            flat_permute(lax.dynamic_index_in_dim(array, (z + step) % 2, 0, False)[0], there[step])
            for step in range(2)
        ]
        return jnp.concatenate(blocks, 0)

    def send_home(array):
        rows = array.shape[0] // 2
        blocks = [flat_permute(array[step * rows : (step + 1) * rows], back[step]) for step in range(2)]
        return blocks

    def in_place(blocks, dtype):
        even = z % 2 == 0
        lower = jnp.where(even, blocks[0], blocks[1])
        upper = jnp.where(even, blocks[1], blocks[0])
        return jnp.stack([lower, upper])[:, None].astype(dtype)

    stream = bring(tri_planes).astype(F32)
    image_rows = bring(images)
    grad_out = bring(cotangent)

    positions = jnp.arange(object_count, dtype=jnp.int32)

    def slot_of(group, level):
        return (level // 2) * groups + group - group % 2 + level % 2

    chosen = jnp.sum(jnp.where(positions == slot_of(n, z), cam_index, 0))
    camera = jnp.dot((positions == chosen).astype(F32), cameras, precision=lax.Precision.HIGHEST)
    modulation = jnp.dot(camera, w_mod.astype(F32), precision=lax.Precision.HIGHEST)
    pieces = [modulation[i * width : (i + 1) * width] for i in range(6)]

    rows = functools.partial(sum_rows, groups=groups, group_index=n)
    across = functools.partial(sum_levels, level=z, depth=depth)
    swap = lambda value: swap_bit(value, 0, groups)

    own_one = dot(image_rows, w_kv_image, 1, 0).astype(BF)
    other_one = swap(own_one)
    normed_one, pull_one = jax.vjp(modnorm, stream, pieces[0], pieces[1])
    hidden_one = normed_one.astype(BF)
    query_one = dot(hidden_one, w_query, 1, 0).astype(BF)
    mixed_one, logs_one = attend(query_one, own_one, other_one)
    stream_one = stream + dot(mixed_one, w_cross_out, 1, 0)
    normed_two, pull_two = jax.vjp(modnorm, stream_one, pieces[2], pieces[3])
    hidden_two = normed_two.astype(BF)
    own_two = dot(hidden_two, w_qkv[:, width:], 1, 0).astype(BF)
    other_two = swap(own_two)
    query_two = dot(hidden_two, w_qkv[:, :width], 1, 0).astype(BF)
    mixed_two, logs_two = attend(query_two, own_two, other_two)
    stream_two = stream_one + dot(mixed_two, w_self_out, 1, 0)
    normed_three, pull_three = jax.vjp(modnorm, stream_two, pieces[4], pieces[5])
    hidden_three = normed_three.astype(BF)
    upper = dot(hidden_three, w_up, 1, 0)
    activated, pull_gelu = jax.vjp(gelu_tanh, upper)
    activated = activated.astype(BF)
    out_home = send_home((stream_two + dot(activated, w_down, 1, 0)).astype(BF))

    total_down = across(rows(activated, grad_out, 0))
    grad_upper = pull_gelu(dot(grad_out, w_down, 1, 1))[0].astype(BF)
    part_two, grad_shift3, grad_scale3 = pull_three(dot(grad_upper, w_up, 1, 1))
    total_up = across(rows(hidden_three, grad_upper, 1))
    grad_stream_two = grad_out.astype(F32) + part_two
    grad_branch_two = grad_stream_two.astype(BF)
    grad_mixed_two = dot(grad_branch_two, w_self_out, 1, 1).astype(BF)
    total_self_out = across(rows(mixed_two, grad_branch_two, 0))
    grad_query_two, dk0, dk1, dv0, dv1 = attend_back(
        query_two, own_two, other_two, mixed_two, grad_mixed_two, logs_two
    )
    grad_keys = (dk0.astype(F32) + swap(dk1).astype(F32)).astype(BF)
    grad_values = (dv0.astype(F32) + swap(dv1).astype(F32)).astype(BF)
    grad_joined = jnp.concatenate([grad_query_two, grad_keys, grad_values], axis=1)
    part_one, grad_shift2, grad_scale2 = pull_two(dot(grad_joined, w_qkv, 1, 1))
    total_qkv = across(rows(hidden_two, grad_joined, 1))
    grad_stream_one = grad_stream_two + part_one
    grad_branch_one = grad_stream_one.astype(BF)
    grad_mixed_one = dot(grad_branch_one, w_cross_out, 1, 1).astype(BF)
    total_cross_out = across(rows(mixed_one, grad_branch_one, 0))
    grad_query_one, dk0, dk1, dv0, dv1 = attend_back(
        query_one, own_one, other_one, mixed_one, grad_mixed_one, logs_one
    )
    part_zero, grad_shift1, grad_scale1 = pull_one(dot(grad_query_one, w_query, 1, 1))
    tri_home = send_home((grad_stream_one + part_zero).astype(BF))
    grad_keys = (dk0.astype(F32) + swap(dk1).astype(F32)).astype(BF)
    grad_values = (dv0.astype(F32) + swap(dv1).astype(F32)).astype(BF)
    grad_pairs = jnp.concatenate([grad_keys, grad_values], axis=1)
    image_home = send_home(dot(grad_pairs, w_kv_image, 1, 1).astype(BF))
    total_query = across(rows(hidden_one, grad_query_one, 1))
    total_kv = across(rows(image_rows, grad_pairs, 0))

    vectors = jnp.concatenate(
        [grad_shift1, grad_scale1, grad_shift2, grad_scale2, grad_shift3, grad_scale3]
    )
    gathered = lax.all_gather(vectors.astype(BF), AXES).astype(F32)
    every = jnp.arange(groups * depth, dtype=jnp.int32)
    slots = slot_of(every // depth, every % depth)
    cams = jnp.sum(jnp.where(slots[:, None] == positions[None, :], cam_index[None, :], 0), 1)
    picked = jnp.dot(
        (cams[:, None] == positions[None, :]).astype(F32), cameras, precision=lax.Precision.HIGHEST
    )
    share = vectors.shape[0] // groups
    mine = lax.dynamic_slice_in_dim(gathered, n * share, share, 1)
    total_mod = lax.dot_general(
        picked, mine, (((0,), (0,)), ((), ())), precision=lax.Precision.HIGHEST, preferred_element_type=F32
    )

    return (
        in_place(out_home, BF),
        in_place(tri_home, F32),
        in_place(image_home, F32),
        total_mod,
        total_query,
        total_kv,
        total_cross_out,
        total_qkv,
        total_self_out,
        total_up,
        total_down,
    )


def solution(mesh):
    tokens = P(None, "obj", "img", None)
    return jax.shard_map(
        local,
        mesh=mesh,
        in_specs=(tokens, tokens) + (P(),) * 10 + (tokens,),
        out_specs=(tokens, tokens, tokens, P(None, "obj")) + (P("obj", None),) * 7,
        check_vma=False,
    )
```
